32 devices in a mesh: parts: 2 (over x), row: 16 (over z, y, core).
Axes of the slice: x: 2, y: 2, z: 4, core: 2. Of those that a mesh axis runs over, the one named last changes fastest.
Arguments:
- sigma_top: bfloat16 [4096, 2048], P(('parts', 'row')), parts along dimension 0, may hold values from -2 to 8, as said below
- panel_par: bfloat16 [4096, 1024], P(('parts', 'row')), parts along dimension 0, may hold values from -0.25 to 0.25
- dinv_par: float32 [2048, 1024], P(('parts', 'row')), parts along dimension 0, may hold values from -2 to 8, as said below
- panel_kid_top: bfloat16 [4, 2048, 1024], P('parts', 'row'), parts along dimension 0, may hold values from -0.25 to 0.25
- panel_kid_par: bfloat16 [4, 1024, 1024], P('parts', 'row'), parts along dimension 0, may hold values from -0.375 to 0.375
- dvar_kid: float32 [4, 1024], P('parts'), parts along dimension 0, may hold values from 0.5 to 2
- mask_par: int32 [16, 4], P('parts'), parts along dimension 0, may hold values 0 or 1
- mask_kid_top: int32 [4, 8, 4], P('parts'), parts along dimension 0, may hold values 0 or 1
- mask_kid_par: int32 [4, 4, 4], P('parts'), parts along dimension 0, may hold values 0 or 1
Outputs:
- cross_par: bfloat16 [4096, 1024], P(('parts', 'row')), parts along dimension 0
- sigma_par: bfloat16 [2048, 1024], P(('parts', 'row')), parts along dimension 0
- cross_kid_top: bfloat16 [4, 2048, 1024], P('parts', 'row'), parts along dimension 0
- cross_kid_par: bfloat16 [4, 1024, 1024], P('parts', 'row'), parts along dimension 0
- variance_kid: float32 [4, 1024], P('parts'), parts along dimension 0
The draws below stay inside these ranges and needn't reach their ends.
There are 2 independent parts, one for each index of `parts`. The reference program is written for one: setup_inputs(seed, part) draws one part's arguments, and reference() takes and returns one part's arrays. A program takes and returns all parts, laid end to end along the dimension named above; each array names one. Nothing has to cross between parts.
Inputs may be any that keep to these rules, and one draw needn't show every extreme that they name: `sigma_top`: symmetric positive definite. `dinv_par`: symmetric positive definite.
All inputs are finite; a program needn't handle non-finite values.
Results may differ from the reference program's by a relative error of at most 0.0052.
Values may be sent and summed in bfloat16 or wider, within the bound.
No kernel may reach another device: no remote copies, remote signals or barrier semaphores. Data moves between devices by JAX's collectives and lax.ppermute only.
A program may use at most 64 MiB of HBM per device.

```python
import math
import jax
import jax.numpy as jnp
from jax import lax

WT = 2048
W1 = 1024
W2 = 1024
BLK = 256
KIDS = 2


def definite(key, width):
    first, second = jax.random.split(key, 2)
    raw = jax.random.normal(first, (width, width), jnp.float32)
    sym = (raw + raw.T) * (0.25 / jnp.sqrt(jnp.float32(width)))
    diag_part = jax.random.uniform(second, (width,), jnp.float32, 1.0, 2.0)
    whole = sym + jnp.diag(diag_part)
    return whole


def draw_sigma_top(key, part):
    return definite(jax.random.fold_in(key, 11), WT).astype(jnp.bfloat16)


def draw_dinv_par(key, part):
    return definite(jax.random.fold_in(key, 23), W1)


def place_ends(entries, key, low, high):
    longest = entries.shape.index(max(entries.shape))
    spots = []
    for shift in (0, 1):
        where = [jax.random.randint(jax.random.fold_in(key, axis), (), 0, length) for axis, length in enumerate(entries.shape)]
        where[longest] = (where[longest] + shift) % entries.shape[longest]
        spots.append(tuple(where))
    return entries.at[spots[0]].set(low).at[spots[1]].set(high)


def block_scale(rng, extent, shards, smallest, high):
    def one(position, parts):
        steps = jax.random.uniform(jax.random.fold_in(jax.random.fold_in(rng, 6), position), (parts,), jnp.float32, smallest / len(shards), high / len(shards))
        return jnp.repeat(jnp.exp(steps), extent[position] // parts).reshape((-1,) + (1,) * (len(extent) - position - 1))

    level = one(*shards[0])
    for cut in shards[1:]:
        level = level * one(*cut)
    return level


def noise(own_key, shape, spread, reach, cuts=(), dtype=jnp.bfloat16):
    entries = jax.random.normal(own_key, shape, jnp.float32) * spread
    if len(cuts) > 0:
        entries = block_scale(own_key, shape, cuts, -0.22, 0.18) * entries
    return jnp.clip(entries, min=-reach, max=reach).astype(dtype)


def setup_inputs(seed: int = 0, part: int = 0) -> dict:
    arg_keys = jax.random.split(jax.random.key(seed), 10)
    part_splits = jax.random.split(jax.random.fold_in(arg_keys[9], part), 10)
    return {
        "sigma_top": draw_sigma_top(jax.random.fold_in(jax.random.fold_in(arg_keys[9], part), 71), part),
        "panel_par": noise(part_splits[1], (WT, W1), (WT // 4) ** -0.5, 0.25, ((0, 16),)),
        "dinv_par": draw_dinv_par(jax.random.fold_in(jax.random.fold_in(arg_keys[9], part), 71), part),
        "panel_kid_top": noise(part_splits[3], (KIDS, WT, W2), (WT // 4) ** -0.5, 0.25, ((1, 16),)),
        "panel_kid_par": noise(part_splits[4], (KIDS, W1, W2), (W1 // 4) ** -0.5, 0.375, ((1, 16),)),
        "dvar_kid": jnp.clip(jnp.exp(jax.random.uniform(part_splits[5], (KIDS, W2), jnp.float32, math.log(0.5), math.log(2.0))), 0.5, 2.0),
        "mask_par": place_ends((jax.random.randint(part_splits[6], (WT // BLK, W1 // BLK), 0, 3) < 2).astype(jnp.int32), jax.random.fold_in(part_splits[6], 1), 0, 1),
        "mask_kid_top": place_ends((jax.random.randint(part_splits[7], (KIDS, WT // BLK, W2 // BLK), 0, 3) < 2).astype(jnp.int32), jax.random.fold_in(part_splits[7], 1), 0, 1),
        "mask_kid_par": place_ends((jax.random.randint(part_splits[8], (KIDS, W1 // BLK, W2 // BLK), 0, 3) < 2).astype(jnp.int32), jax.random.fold_in(part_splits[8], 1), 0, 1),
    }


def widen(mask):
    grown = jnp.repeat(jnp.repeat(mask, BLK, axis=-2), BLK, axis=-1)
    return grown.astype(jnp.bfloat16)


def reference(sigma_top, panel_par, dinv_par, panel_kid_top, panel_kid_par, dvar_kid, mask_par, mask_kid_top, mask_kid_par):
    high = lax.Precision.HIGHEST
    par_masked = panel_par * widen(mask_par)
    kid_top_masked = panel_kid_top * widen(mask_kid_top)
    kid_par_masked = panel_kid_par * widen(mask_kid_par)
    cross_par = jnp.dot(sigma_top, par_masked, preferred_element_type=jnp.float32).astype(jnp.bfloat16)
    sigma_par = (dinv_par + jnp.dot(par_masked.T, cross_par, preferred_element_type=jnp.float32)).astype(jnp.bfloat16)
    sig_wide = sigma_top.astype(jnp.float32)
    cross_wide = cross_par.astype(jnp.float32)
    spar_wide = sigma_par.astype(jnp.float32)
    ktop_wide = kid_top_masked.astype(jnp.float32)
    kpar_wide = kid_par_masked.astype(jnp.float32)
    kid_top = jnp.einsum("ac,kcw->kaw", sig_wide, ktop_wide, precision=high)
    kid_top = kid_top + jnp.einsum("ap,kpw->kaw", cross_wide, kpar_wide, precision=high)
    cross_kid_top = kid_top.astype(jnp.bfloat16)
    kid_par = jnp.einsum("ap,kaw->kpw", cross_wide, ktop_wide, precision=high)
    kid_par = kid_par + jnp.einsum("pq,kqw->kpw", spar_wide, kpar_wide, precision=high)
    cross_kid_par = kid_par.astype(jnp.bfloat16)
    variance_kid = dvar_kid + jnp.sum(ktop_wide * cross_kid_top.astype(jnp.float32), axis=1)
    variance_kid = variance_kid + jnp.sum(kpar_wide * cross_kid_par.astype(jnp.float32), axis=1)
    return cross_par, sigma_par, cross_kid_top, cross_kid_par, variance_kid
```

```python
import jax
import jax.numpy as jnp
from jax import lax
from jax.sharding import PartitionSpec as P

F32 = jnp.float32
BF16 = jnp.bfloat16


def mask_rows(mask, rows, width, height, position):
    high = height // mask.shape[-2]
    wide = width // mask.shape[-1]
    if high % rows == 0:
        picked = lax.dynamic_slice_in_dim(mask, position * rows // high, 1, axis=mask.ndim - 2)
    else:
        index = (position * rows + jnp.arange(rows, dtype=jnp.int32)) // high
        picked = jnp.take(mask, index, axis=mask.ndim - 2)
    return jnp.repeat(picked.astype(BF16), wide, axis=-1)


def dot(a, b):
    return jnp.dot(a, b, preferred_element_type=F32)


def dot_t(a, b):
    return lax.dot_general(a, b, (((0,), (0,)), ((), ())), preferred_element_type=F32)


def make_shards(n):
    Q = 4 if n % 4 == 0 else n
    Z = n // Q

    def shards(sigma_top, panel_par, dinv_par, panel_kid_top, panel_kid_par, dvar_kid,
               mask_par, mask_kid_top, mask_kid_par):
        t, WT = sigma_top.shape
        p, W1 = dinv_par.shape
        kids, _, W2 = panel_kid_top.shape
        per_kid = Q // kids
        w = kids * W2 // Q
        pg = Q * p
        pos = lax.axis_index("row")
        z = pos // Q
        q = pos % Q

        def permute(x, pairs):
            return lax.ppermute(x, "row", pairs)

        def in_group(x, k, zs=None):
            zs = range(Z) if zs is None else zs
            return permute(x, [(a * Q + b, a * Q + (b ^ k)) for a in zs for b in range(Q)])

        def between(x, zpairs):
            return permute(x, [(a * Q + b, c * Q + b) for a, c in zpairs for b in range(Q)])

        def unxor(pieces):
            pieces = list(pieces)
            bit = 1
            while bit < Q:
                flag = (q & bit) != 0
                pieces = [jnp.where(flag, pieces[k ^ bit], pieces[k]) for k in range(Q)]
                bit *= 2
            return pieces

        def pair_gather(x, zs=None):
            first = jnp.concatenate([x, in_group(x, 2, zs)], axis=0)
            return first, in_group(first, 1, zs)

        def line(x):
            out = []
            up, down = x, x
            for s in range(1, Z):
                up = between(up, [(a, a + 1) for a in range(s - 1, Z - 1)])
                down = between(down, [(a, a - 1) for a in range(1, Z - s + 1)])
                if 2 * s < Z:
                    out.append((up, jnp.where(z >= s, z - s, Z), range(s, Z)))
                    out.append((down, jnp.where(z + s < Z, z + s, Z), range(0, Z - s)))
                else:
                    low = z + s < Z
                    out.append((jnp.where(low, down, up),
                                jnp.where(low, z + s, jnp.where(z >= s, z - s, Z)),
                                [a for a in range(Z) if a >= s or a + s < Z]))
            return out

        def collect(own, blocks, rows):
            full = jnp.zeros(((Z + 1) * rows, own.shape[1]), own.dtype)
            full = lax.dynamic_update_slice(full, own, (z * rows, 0))
            for blk, zi, _ in blocks:
                full = lax.dynamic_update_slice(full, blk, (zi * rows, 0))
            return full[:Z * rows]

        par_d = panel_par * mask_rows(mask_par, t, W1, WT, pos)
        kt_d = panel_kid_top * mask_rows(mask_kid_top, t, W2, WT, pos)
        kp_d = panel_kid_par * mask_rows(mask_kid_par, p, W2, W1, pos)

        par = jnp.zeros(((Z + 1) * Q * t, W1), BF16)
        for blk, zi, zs in [(par_d, z, range(Z))] + line(par_d):
            pa, pb = pair_gather(blk, zs)
            for half, ks in ((pa, (0, 2)), (pb, (1, 3))):
                for i, k in enumerate(ks):
                    par = lax.dynamic_update_slice(
                        par, half[i * t:(i + 1) * t], ((zi * Q + (q ^ k)) * t, 0))
        par = par[:WT]

        def chunks(x):
            r = x.shape[1]
            c = x.reshape(kids, r, per_kid, w).transpose(0, 2, 1, 3).reshape(Q, r, w)
            own = lax.dynamic_index_in_dim(c, q, 0, keepdims=False)
            return [own] + [in_group(lax.dynamic_index_in_dim(c, q ^ k, 0, keepdims=False), k)
                            for k in range(1, Q)]

        kt_pieces = chunks(kt_d)
        kt_g = jnp.concatenate(unxor(kt_pieces), axis=0)
        kp_pieces = chunks(kp_d)
        kp_g = jnp.concatenate(unxor(kp_pieces), axis=0)
        kt = collect(kt_g, line(kt_g), Q * t)
        kp = collect(kp_g, line(kp_g), Q * p)

        sig_a, sig_b = pair_gather(sigma_top)
        dinv_a, dinv_b = pair_gather(dinv_par)
        dinv_g = jnp.concatenate(
            unxor([dinv_a[:p], dinv_b[:p], dinv_a[p:], dinv_b[p:]]), axis=0)

        cross_par = dot(sigma_top, par).astype(BF16)
        cross_a, cross_b = pair_gather(cross_par)

        mine = jnp.zeros((Z, t, pg), BF16)
        mine = lax.dynamic_update_slice(
            mine, lax.dynamic_slice(cross_par, (0, z * pg), (t, pg))[None], (z, 0, 0))
        for m in range(1, Z):
            got = between(lax.dynamic_slice(cross_par, (0, (z + m) % Z * pg), (t, pg)),
                          [(a, (a + m) % Z) for a in range(Z)])
            mine = lax.dynamic_update_slice(mine, got[None], ((z - m) % Z, 0, 0))
        ta, tb = pair_gather(mine)
        turned = jnp.stack(unxor([ta[:Z], tb[:Z], ta[Z:], tb[Z:]]), axis=1).reshape(WT, pg)

        sigma_g = (dinv_g + dot_t(turned, par)).astype(BF16)
        sigma_par = lax.dynamic_slice(sigma_g, (q * p, 0), (p, W1))

        top_a = (dot(sig_a, kt) + dot(cross_a, kp)).astype(BF16)
        top_b = (dot(sig_b, kt) + dot(cross_b, kp)).astype(BF16)
        low = (dot_t(turned, kt) + dot(sigma_g, kp)).astype(BF16)

        top_k = [top_a[:t], top_b[:t], top_a[t:], top_b[t:]]
        top_out = unxor([top_k[0]] + [in_group(top_k[k], k) for k in range(1, Q)])
        low_q = low.reshape(Q, p, w)
        low_out = unxor([lax.dynamic_index_in_dim(low_q, q, 0, keepdims=False)] + [
            in_group(lax.dynamic_index_in_dim(low_q, q ^ k, 0, keepdims=False), k)
            for k in range(1, Q)])

        def whole(pieces):
            r = pieces[0].shape[0]
            x = jnp.stack(pieces, 0).reshape(kids, per_kid, r, w)
            return x.transpose(0, 2, 1, 3).reshape(kids, r, W2)

        cross_kid_top = whole(top_out)
        cross_kid_par = whole(low_out)

        var = sum(jnp.sum(kt_pieces[k].astype(F32) * top_k[k].astype(F32), axis=0)
                  for k in range(Q))
        var = var + jnp.sum(kp_g.astype(F32) * low.astype(F32), axis=0)
        parts = jnp.zeros((Z, w), F32)
        parts = lax.dynamic_update_slice(parts, var[None], (z, 0))
        for m in range(1, Z):
            got = between(var, [(a, (a + m) % Z) for a in range(Z)])
            parts = lax.dynamic_update_slice(parts, got[None], ((z - m) % Z, 0))
        summed = jnp.sum(parts, axis=0)
        every = jnp.concatenate(unxor([summed] + [in_group(summed, k) for k in range(1, Q)]))
        variance_kid = dvar_kid + every.reshape(kids, W2)
        return cross_par, sigma_par, cross_kid_top, cross_kid_par, variance_kid

    return shards


def solution(mesh):
    rows = P(("parts", "row"), None)
    kid = P("parts", "row", None)
    return jax.shard_map(
        make_shards(mesh.shape["row"]),
        mesh=mesh,
        in_specs=(rows, rows, rows, kid, kid, P("parts", None), P("parts", None),
                  P("parts", None, None), P("parts", None, None)),
        out_specs=(rows, rows, kid, kid, P("parts", None)),
        check_vma=False,
    )
```

```python
import functools

import jax
import jax.numpy as jnp
from jax import lax
from jax.experimental import pallas as pl
from jax.experimental.pallas import tpu as pltpu
from jax.sharding import PartitionSpec as P


F32 = jnp.float32
BF16 = jnp.bfloat16
Q = 4
ORDER = (0, 2, 1, 3)
EXTRA = 16


def mask_rows(mask, rows, width, height, position):
    high = height // mask.shape[-2]
    wide = width // mask.shape[-1]
    if high % rows == 0:
        picked = lax.dynamic_slice_in_dim(mask, position * rows // high, 1, axis=mask.ndim - 2)
    else:
        index = (position * rows + jnp.arange(rows, dtype=jnp.int32)) // high
        picked = jnp.take(mask, index, axis=mask.ndim - 2)
    return jnp.repeat(picked.astype(BF16), wide, axis=-1)


def dot(a, b):
    return jnp.dot(a, b, preferred_element_type=F32)


def dot_t(a, b):
    return lax.dot_general(a, b, (((0,), (0,)), ((), ())), preferred_element_type=F32)


def after(x, *deps):
    return lax.optimization_barrier((x,) + deps)[0]


def split3(x):
    high = x.astype(BF16)
    rest = x - high.astype(F32)
    mid = rest.astype(BF16)
    return high, mid, (rest - mid.astype(F32)).astype(BF16)


def call(body, out_shape, args, flops, scratch=(), smem=1):
    size = sum(a.size * a.dtype.itemsize for a in args)
    vmem = pl.BlockSpec(memory_space=pltpu.VMEM)
    return pl.pallas_call(
        body,
        out_shape=out_shape,
        in_specs=[pl.BlockSpec(memory_space=pltpu.SMEM)] * smem + [vmem] * (len(args) - smem),
        out_specs=jax.tree.map(lambda _: vmem, out_shape),
        scratch_shapes=list(scratch),
        cost_estimate=pl.CostEstimate(flops=flops, bytes_accessed=size, transcendentals=0),
        compiler_params=pltpu.CompilerParams(vmem_limit_bytes=48 * 2 ** 20),
    )(*args)


def place(own, ups, downs, z, Z):
    out = [(own, z, None)]
    for s, (u, d) in enumerate(zip(ups, downs), 1):
        out.append((u, z - s, z >= s))
        out.append((d, z + s, z + s < Z))
    return out


def when(flag, f):
    if flag is None:
        f()
    else:
        pl.when(flag)(f)


def fill(slots, z, q, Z, full, step, off, rows):
    n = (len(slots) - 1) // 2
    for x, zi, flag in place(slots[0], slots[1:1 + n], slots[1 + n:], z, Z):
        def put(x=x, zi=zi):
            for k in range(Q):
                at = pl.multiple_of((zi * Q + (q ^ k)) * rows, rows)
                full[pl.ds(at, rows), :] = x[k * step + off:k * step + off + rows, :]

        when(flag, put)


def par_body(t, v, wide, high, where_ref, mask_ref, x_ref, *outs):
    pos, q = where_ref[2], where_ref[1]
    row = pos * t // high
    step = min(v, wide)
    for k in range(Q):
        peer = q ^ k
        for c in range(0, v, step):
            keep = mask_ref[row, (peer * v + c) // wide] != 0
            x = x_ref[:, pl.ds(pl.multiple_of(peer * v + c, step), step)]
            outs[k][:, c:c + step] = jnp.where(keep, x, jnp.zeros_like(x))


def kid_body(t, p, u, halves, per_kid, wide, high_t, high_p, where_ref, mt_ref, mp_ref, xt_ref,
             xp_ref, *outs):
    pos, q = where_ref[2], where_ref[1]
    step = min(u, wide)
    for k in range(Q):
        peer = q ^ k
        one = peer // per_kid
        for i in range(halves):
            for c in range(0, u, step):
                col = (peer % per_kid) * (u * halves) + i * u + c
                at = pl.ds(pl.multiple_of(col, step), step)
                for m_ref, x_ref, high, r, lo in ((mt_ref, xt_ref, high_t, t, 0),
                                                  (mp_ref, xp_ref, high_p, p, t)):
                    keep = m_ref[one, pos * r // high, col // wide] != 0
                    x = x_ref[one, :, at]
                    outs[k][i, lo:lo + r, c:c + step] = jnp.where(keep, x, jnp.zeros_like(x))


def cross_body(Z, t, where_ref, sa_ref, sb_ref, *refs):
    slots, out_ref, full = refs[:-2], refs[-2], refs[-1]
    z, q = where_ref[0], where_ref[1]
    fill(slots, z, q, Z, full, t, 0, t)
    for i, k in enumerate(ORDER):
        s = (sa_ref, sb_ref)[i // 2]
        at = pl.ds(pl.multiple_of((q ^ k) * t, t), t)
        out_ref[at, :] = dot(s[(i % 2) * t:(i % 2 + 1) * t, :], full[...]).astype(BF16)


def sigma_body(Z, t, p, v, where_ref, da_ref, db_ref, ta_ref, tb_ref, *refs):
    slots, out_ref, full, acc = refs[:-3], refs[-3], refs[-2], refs[-1]
    z, q = where_ref[0], where_ref[1]
    g = Q * t
    fill(slots, z, q, Z, full, t, 0, t)
    cols = pl.ds(pl.multiple_of(q * v, v), v)
    for i, k in enumerate(ORDER):
        d = (da_ref, db_ref)[i // 2]
        at = pl.ds(pl.multiple_of((q ^ k) * p, p), p)
        acc[at, :] = d[(i % 2) * p:(i % 2 + 1) * p, cols]
    for i, k in enumerate(ORDER):
        x = (ta_ref, tb_ref)[i // 2]
        at = pl.ds(pl.multiple_of((q ^ k) * g, g), g)
        acc[...] += dot_t(x[(i % 2) * g:(i % 2 + 1) * g, :], full[at, :])
    out_ref[...] = acc[...].astype(BF16)


def pre_body(Z, t, p, u, v, first, where_ref, sa_ref, sb_ref, ca_ref, cb_ref, *refs):
    refs = list(refs)
    kp, kt = refs.pop(), refs.pop()
    if first:
        cross_ref = refs.pop()
    top = refs.pop()
    slots = refs
    z, q = where_ref[0], where_ref[1]
    g, h = Q * t, Q * p
    far = jnp.where(z + Z - 1 < Z, z + Z - 1, z - Z + 1)

    def clear():
        kt[pl.ds(pl.multiple_of(far * g, g), g), :] = jnp.zeros((g, u), BF16)
        kp[pl.ds(pl.multiple_of(far * h, h), h), :] = jnp.zeros((h, u), BF16)

    pl.when(far >= 0)(clear)
    fill(slots, z, q, Z, kt, t + p, 0, t)
    fill(slots, z, q, Z, kp, t + p, t, p)
    for i, k in enumerate(ORDER):
        peer = q ^ k
        s = (sa_ref, sb_ref)[i // 2]
        c = dot(s[(i % 2) * t:(i % 2 + 1) * t, :], kt[...])
        for j, m in enumerate(ORDER):
            x = (ca_ref, cb_ref)[j // 2]
            at = pl.ds(pl.multiple_of((q ^ m) * v, v), v)
            mine = pl.ds(pl.multiple_of((j % 2) * g + peer * t, t), t)
            c = c + dot(x[mine, :], kp[at, :])
        top[i * t:(i + 1) * t, :] = c
    if first:
        for j, m in enumerate(ORDER):
            at = pl.ds(pl.multiple_of((q ^ m) * v, v), v)
            x = (ca_ref, cb_ref)[j // 2]
            cross_ref[:, at] = x[pl.ds(pl.multiple_of((j % 2) * g + q * t, t), t), :]


def low_body(Z, t, p, u, v, first, where_ref, ta_ref, tb_ref, pa_ref, pb_ref, *refs):
    refs = list(refs)
    kp, kt = refs.pop(), refs.pop()
    if first:
        sp_ref = refs.pop()
    low = refs.pop()
    slots = refs
    z, q = where_ref[0], where_ref[1]
    g, h = Q * t, Q * p
    far = jnp.where(z + Z - 1 < Z, z + Z - 1, z - Z + 1)

    def clear():
        kt[pl.ds(pl.multiple_of(far * g, g), g), :] = jnp.zeros((g, u), BF16)
        kp[pl.ds(pl.multiple_of(far * h, h), h), :] = jnp.zeros((h, u), BF16)

    pl.when(far >= 0)(clear)
    fill(slots, z, q, Z, kt, t + p, 0, t)
    fill(slots, z, q, Z, kp, t + p, t, p)
    for i, k in enumerate(ORDER):
        x = (ta_ref, tb_ref)[i // 2]
        at = pl.ds(pl.multiple_of((q ^ k) * g, g), g)
        part = dot_t(x[(i % 2) * g:(i % 2 + 1) * g, :], kt[at, :])
        low[...] = part if i == 0 else low[...] + part
        x = (pa_ref, pb_ref)[i // 2]
        at = pl.ds(pl.multiple_of((q ^ k) * v, v), v)
        low[...] += dot(x[(i % 2) * h:(i % 2 + 1) * h, :], kp[at, :])
    if first:
        for j, m in enumerate(ORDER):
            at = pl.ds(pl.multiple_of((q ^ m) * v, v), v)
            x = (pa_ref, pb_ref)[j // 2]
            sp_ref[:, at] = x[pl.ds(pl.multiple_of((j % 2) * h + q * p, p), p), :]


def post_body(Z, t, p, u, where_ref, sa_ref, sb_ref, ca_ref, cb_ref, ta_ref, tb_ref,
              pa_ref, pb_ref, top_in, low_in, own, up_ref, down_ref, *refs):
    outs, (var_ref, top, low, kt, kp) = refs[:Q], refs[Q:]
    z, q = where_ref[0], where_ref[1]
    g, h = Q * t, Q * p
    top[...] = top_in[...]
    low[...] = low_in[...]
    for x, zi, flag in ((up_ref, z - (Z - 1), z >= Z - 1), (down_ref, z + (Z - 1), z <= 0)):
        def put(x=x, zi=zi):
            for k in range(Q):
                at = pl.ds(pl.multiple_of((q ^ k) * t, t), t)
                kt[at, :] = x[k * (t + p):k * (t + p) + t, :]
                at = pl.ds(pl.multiple_of((q ^ k) * p, p), p)
                kp[at, :] = x[k * (t + p) + t:(k + 1) * (t + p), :]
            cols = pl.ds(pl.multiple_of(zi * g, g), g)
            for j, m in enumerate(ORDER):
                def add(j=j):
                    side, lo = j // 2, j % 2
                    low[...] += dot_t((ta_ref, tb_ref)[side][lo * g:(lo + 1) * g, :], kt[...])
                    low[...] += dot((pa_ref, pb_ref)[side][lo * h:(lo + 1) * h, :], kp[...])
                    for i, k in enumerate(ORDER):
                        mine = pl.ds(pl.multiple_of(lo * g + (q ^ k) * t, t), t)
                        s = (sa_ref, sb_ref)[i // 2]
                        rows = slice(i * t, (i + 1) * t)
                        top[rows, :] += (
                            dot(s[(i % 2) * t:(i % 2 + 1) * t, cols], kt[...])
                            + dot((ca_ref, cb_ref)[side][mine, :], kp[...]))

                pl.when(zi == q ^ m)(add)

        pl.when(flag)(put)
    var = jnp.zeros((1, u), F32)
    for i, k in enumerate(ORDER):
        c = top[i * t:(i + 1) * t, :].astype(BF16)
        outs[k][:t, :] = c
        x = own[k * (t + p):k * (t + p) + t, :]
        var = var + jnp.sum(x.astype(F32) * c.astype(F32), axis=0, keepdims=True)
        c = low[pl.ds(pl.multiple_of((q ^ k) * p, p), p), :].astype(BF16)
        outs[k][t:, :] = c
        x = own[k * (t + p) + t:(k + 1) * (t + p), :]
        var = var + jnp.sum(x.astype(F32) * c.astype(F32), axis=0, keepdims=True)
    var_ref[...] = var


def out_body(t, p, u, halves, per_kid, where_ref, *refs):
    ins, (top_ref, low_ref) = refs[:-2], refs[-2:]
    q = where_ref[1]
    for i in range(halves):
        for k in range(Q):
            x = ins[i * Q + k]
            peer = q ^ k
            one = peer // per_kid
            at = pl.ds(pl.multiple_of((peer % per_kid) * (u * halves) + i * u, u), u)
            top_ref[one, :, at] = x[:t, :]
            low_ref[one, :, at] = x[t:t + p, :]


def line_sum_body(Z, where_ref, *refs):
    ins, out_ref, rows = refs[:-2], refs[-2], refs[-1]
    for m in range(Z):
        rows[pl.ds(lax.rem(where_ref[0] - m + Z, Z), 1), :] = ins[m][...]
    total = rows[0:1, :]
    for k in range(1, Z):
        total = total + rows[k:k + 1, :]
    out_ref[...] = total


def variance_body(w, per_kid, where_ref, dvar_ref, *refs):
    ins, out_ref = refs[:-1], refs[-1]
    for k in range(Q):
        peer = where_ref[1] ^ k
        at = pl.ds(pl.multiple_of((peer % per_kid) * w, w), w)
        row = pl.ds(peer // per_kid, 1)
        out_ref[row, at] = dvar_ref[row, at] + ins[k][...]


def make_shards(n):
    Z = n // Q

    def plain(sigma_top, panel_par, dinv_par, panel_kid_top, panel_kid_par, dvar_kid,
              mask_par, mask_kid_top, mask_kid_par):
        t, WT = sigma_top.shape
        p, W1 = dinv_par.shape
        kids, _, W2 = panel_kid_top.shape
        per_kid = Q // kids
        w = kids * W2 // Q
        v = W1 // Q
        g, h = Q * t, Q * p
        halves = 2
        u = w // halves
        pos = lax.axis_index("row")
        z = pos // Q
        q = pos % Q

        def permute(x, pairs):
            return lax.ppermute(x, "row", pairs)

        def in_group(x, k):
            pairs = [(a * Q + b, a * Q + (b ^ k)) for a in range(Z) for b in range(Q)]
            return permute(x, pairs)

        def between(x, zpairs):
            return permute(x, [(a * Q + b, c * Q + b) for a, c in zpairs for b in range(Q)])

        def unxor(pieces, at=None):
            at = q if at is None else at
            pieces = list(pieces)
            bit = 1
            while bit < Q:
                flag = (at & bit) != 0
                pieces = [jnp.where(flag, pieces[k ^ bit], pieces[k]) for k in range(Q)]
                bit *= 2
            return pieces

        def pair_gather(x):
            first = jnp.concatenate([x, in_group(x, 2)], axis=0)
            return first, in_group(first, 1)

        def gather4(x):
            first, second = pair_gather(x)
            r = x.shape[0]
            return unxor([first[:r], second[:r], first[r:], second[r:]])

        def hop(x, s, way):
            if way > 0:
                return between(x, [(a, a + 1) for a in range(s - 1, Z - 1)])
            return between(x, [(a, a - 1) for a in range(1, Z - s + 1)])

        def pieces_of(c):
            own = lax.dynamic_index_in_dim(c, q, 0, keepdims=False)
            return [own] + [in_group(lax.dynamic_index_in_dim(c, q ^ k, 0, keepdims=False), k) for k in range(1, Q)]

        def assemble(own, ups, downs):
            r = own.shape[0]
            full = jnp.zeros(((Z + 1) * r,) + own.shape[1:], own.dtype)
            for x, zi, flag in place(own, ups, downs, z, Z):
                zi = zi if flag is None else jnp.where(flag, zi, Z)
                full = lax.dynamic_update_slice(full, x, (zi * r, 0))
            return full[:Z * r]

        par_d = panel_par * mask_rows(mask_par, t, W1, WT, pos)
        par_g = jnp.concatenate(
            unxor(pieces_of(par_d.reshape(t, Q, v).transpose(1, 0, 2))), axis=0)

        def chunks(x):
            r = x.shape[1]
            return x.reshape(kids, r, per_kid, w).transpose(0, 2, 1, 3).reshape(Q, r, w)

        kt_d = after(panel_kid_top, par_d) * mask_rows(mask_kid_top, t, W2, WT, pos)
        kp_d = panel_kid_par * mask_rows(mask_kid_par, p, W2, W1, pos)
        kid = unxor(pieces_of(jnp.concatenate([chunks(kt_d), chunks(kp_d)], axis=1)))
        kid_g = jnp.concatenate([x[:t] for x in kid] + [x[t:] for x in kid], axis=0)
        own = [kid_g[:, i * u:(i + 1) * u] for i in range(halves)]

        pu, pd = [], []
        ku, kd = [[] for _ in own], [[] for _ in own]
        for s in range(1, Z):
            pu.append(hop(pu[-1] if pu else par_g, s, 1))
            pd.append(hop(pd[-1] if pd else par_g, s, -1))
        for s in range(1, Z):
            for i in range(halves):
                ku[i].append(hop(ku[i][-1] if s > 1 else own[i], s, 1))
                kd[i].append(hop(kd[i][-1] if s > 1 else own[i], s, -1))

        sig_a, sig_b = pair_gather(after(sigma_top, kid_g))
        dinv_pieces = gather4(after(dinv_par, sig_a))
        dinv_c = jnp.concatenate(
            [lax.dynamic_slice(x, (0, q * v), (p, v)) for x in dinv_pieces], axis=0)

        par = assemble(par_g, pu, pd)
        cross_c = jnp.concatenate([dot(sig_a, par), dot(sig_b, par)], 0).astype(BF16)

        if Z == Q:
            turn = permute(cross_c, [(a * Q + b, b * Q + a) for a in range(Z) for b in range(Q)])
            turn = jnp.concatenate(unxor([turn[ORDER.index(k) * t:(ORDER.index(k) + 1) * t]
                                          for k in range(Q)], z), axis=0)
            turned = jnp.concatenate(gather4(turn), axis=0)

        ca, cb = pair_gather(cross_c)
        chunk = (ca[:g], cb[:g], ca[g:], cb[g:])

        def cross_rows(r):
            at = [ORDER.index(r ^ k) * t for k in range(Q)]
            return jnp.concatenate(
                unxor([chunk[k][at[k]:at[k] + t] for k in range(Q)]), axis=1)

        cross_par = cross_rows(0)
        cross_g = jnp.concatenate([cross_par] + [cross_rows(r) for r in ORDER[1:]], axis=0)
        if Z != Q:
            turn = lax.all_to_all(cross_par, "row", split_axis=1, concat_axis=0, tiled=True)
            turned = jnp.concatenate(gather4(turn), axis=1)

        sigma_c = (dinv_c + dot_t(turned, par)).astype(BF16)
        sigma_g = jnp.concatenate(gather4(sigma_c), axis=1)
        sigma_par = lax.dynamic_slice(sigma_g, (q * p, 0), (p, W1))

        def final(i):
            full = assemble(own[i], ku[i], kd[i]).reshape(Z, g + h, u)
            kt, kp = full[:, :g].reshape(WT, u), full[:, g:].reshape(W1, u)
            sig = jnp.concatenate([sig_a, sig_b], 0)
            top = (dot(sig, kt) + dot(cross_g, kp)).astype(BF16).reshape(Q, t, u)
            low = (dot_t(turned, kt) + dot(sigma_g, kp)).astype(BF16).reshape(Q, p, u)
            top = jnp.stack([top[ORDER.index(k)] for k in range(Q)])
            low = jnp.stack([lax.dynamic_index_in_dim(low, q ^ k, 0, False) for k in range(Q)])
            mine = own[i].astype(F32)
            var = jnp.zeros((1, u), F32)
            for k in range(Q):
                x = lax.dynamic_slice(mine, ((q ^ k) * t, 0), (t, u))
                y = lax.dynamic_slice(mine, (g + (q ^ k) * p, 0), (p, u))
                var = var + jnp.sum(x * top[k].astype(F32), 0, keepdims=True)
                var = var + jnp.sum(y * low[k].astype(F32), 0, keepdims=True)
            tail = jnp.concatenate(split3(var) + (jnp.zeros((EXTRA - 3, u), BF16),), axis=0)
            return jnp.concatenate([top, low, jnp.broadcast_to(tail, (Q, EXTRA, u))], axis=1)

        outs = []
        for i in range(halves):
            c = final(i)
            outs.append(unxor([c[0]] + [in_group(c[k], k) for k in range(1, Q)]))

        def whole(first, last):
            x = jnp.stack([jnp.stack([outs[i][j][first:last] for i in range(halves)], 0)
                           for j in range(Q)], 0)
            x = x.reshape(kids, per_kid, halves, last - first, u)
            return x.transpose(0, 3, 1, 2, 4).reshape(kids, last - first, W2)

        cross_kid_top = whole(0, t)
        cross_kid_par = whole(t, t + p)
        three = whole(t + p, t + p + 3).astype(F32)
        part = three[:, 0] + three[:, 1] + three[:, 2]
        sums = jnp.zeros((Z, kids, W2), F32)
        sums = lax.dynamic_update_slice(sums, part[None], (z, 0, 0))
        for m in range(1, Z):
            other = between(part, [(a, (a + m) % Z) for a in range(Z)])
            sums = lax.dynamic_update_slice(sums, other[None], ((z - m) % Z, 0, 0))
        variance_kid = dvar_kid + jnp.sum(sums, axis=0)
        return cross_par, sigma_par, cross_kid_top, cross_kid_par, variance_kid

    def choose(*args):
        sigma_top, _, dinv_par, kid_top = args[:4]
        t, WT = sigma_top.shape
        p, W1 = dinv_par.shape
        masks = args[6:]
        u = kid_top.shape[0] * kid_top.shape[2] // Q // 2
        wide = kid_top.shape[2] // masks[1].shape[-1]
        good = (Z == Q and t % 16 == 0 and p % 16 == 0 and (W1 // Q) % 128 == 0 and u % 128 == 0
                and (WT // masks[0].shape[0]) % t == 0 and (W1 // masks[2].shape[1]) % p == 0
                and wide % 128 == 0 and Q % kid_top.shape[0] == 0)
        return (fast if good else plain)(*args)

    def fast(sigma_top, panel_par, dinv_par, panel_kid_top, panel_kid_par, dvar_kid,
             mask_par, mask_kid_top, mask_kid_par):
        t, WT = sigma_top.shape
        p, W1 = dinv_par.shape
        kids, _, W2 = panel_kid_top.shape
        per_kid = Q // kids
        w = kids * W2 // Q
        v = W1 // Q
        g, h = Q * t, Q * p
        halves = 2
        u = w // halves
        pos = lax.axis_index("row")
        z = pos // Q
        q = pos % Q
        where = jnp.stack([z, q, pos]).astype(jnp.int32)

        def permute(x, pairs):
            return lax.ppermute(x, "row", pairs)

        def in_group(x, k):
            pairs = [(a * Q + b, a * Q + (b ^ k)) for a in range(Z) for b in range(Q)]
            return permute(x, pairs)

        def between(x, zpairs):
            return permute(x, [(a * Q + b, c * Q + b) for a, c in zpairs for b in range(Q)])

        def pair_gather(x):
            first = jnp.concatenate([x, in_group(x, 2)], axis=0)
            return first, in_group(first, 1)

        def hop(x, s, way):
            if way > 0:
                return between(x, [(a, a + 1) for a in range(s - 1, Z - 1)])
            return between(x, [(a, a - 1) for a in range(1, Z - s + 1)])

        def shape(*dims):
            return jax.ShapeDtypeStruct(dims, BF16)

        wide = W1 // mask_par.shape[1]
        sent = call(functools.partial(par_body, t, v, wide, WT // mask_par.shape[0]),
                    [shape(t, v)] * Q, [where, mask_par, panel_par], 1, smem=2)
        par_g = jnp.concatenate(
            [sent[0]] + [in_group(sent[k], k) for k in range(1, Q)], axis=0)

        wide = W2 // mask_kid_top.shape[2]
        sent = call(functools.partial(kid_body, t, p, u, halves, per_kid, wide,
                                      WT // mask_kid_top.shape[1], W1 // mask_kid_par.shape[1]),
                    [shape(halves, t + p, u)] * Q,
                    [where, mask_kid_top, mask_kid_par, after(panel_kid_top, sent[0]),
                     panel_kid_par], 1, smem=3)
        got = [sent[0]] + [in_group(sent[k], k) for k in range(1, Q)]
        own = [jnp.concatenate([x[i] for x in got], axis=0) for i in range(halves)]

        pu, pd = [], []
        ku, kd = [[] for _ in own], [[] for _ in own]
        for s in range(1, Z):
            pu.append(hop(pu[-1] if pu else par_g, s, 1))
            pd.append(hop(pd[-1] if pd else par_g, s, -1))
        for s in range(1, Z):
            for i in range(halves):
                ku[i].append(hop(ku[i][-1] if s > 1 else own[i], s, 1))
                kd[i].append(hop(kd[i][-1] if s > 1 else own[i], s, -1))

        sig_a, sig_b = pair_gather(sigma_top)
        dinv_a, dinv_b = pair_gather(dinv_par)

        cross_c = call(functools.partial(cross_body, Z, t), shape(g, v),
                       [where, sig_a, sig_b, par_g] + pu + pd, 2 * g * WT * v,
                       [pltpu.VMEM((WT, v), BF16)])
        turn = permute(cross_c, [(a * Q + b, b * Q + a) for a in range(Z) for b in range(Q)])
        turned_a, turned_b = pair_gather(turn)
        cross_a, cross_b = pair_gather(cross_c)

        sigma_c = call(functools.partial(sigma_body, Z, t, p, v), shape(h, v),
                       [where, dinv_a, dinv_b, turned_a, turned_b, par_g] + pu + pd,
                       2 * h * WT * v, [pltpu.VMEM((WT, v), BF16), pltpu.VMEM((h, v), F32)])
        sp_a, sp_b = pair_gather(sigma_c)

        sides = [where, sig_a, sig_b, cross_a, cross_b, turned_a, turned_b, sp_a, sp_b]
        wide32 = [jax.ShapeDtypeStruct((g, u), F32), jax.ShapeDtypeStruct((h, u), F32)]
        outs, var, tops, lows = [], [], [], []
        scratch = [pltpu.VMEM((WT, u), BF16), pltpu.VMEM((W1, u), BF16)]
        for i in range(halves):
            res = call(functools.partial(pre_body, Z, t, p, u, v, i == 0),
                       wide32[:1] + ([shape(t, W1)] if i == 0 else []),
                       [where, sig_a, sig_b, cross_a, cross_b, own[i]] + ku[i][:-1] + kd[i][:-1],
                       2 * g * (WT + W1) * u, scratch)
            tops.append(res[0])
            if i == 0:
                cross_par = res[1]
        for i in range(halves):
            res = call(functools.partial(low_body, Z, t, p, u, v, i == 0),
                       wide32[1:] + ([shape(p, W1)] if i == 0 else []),
                       [where, turned_a, turned_b, sp_a, sp_b, own[i]] + ku[i][:-1] + kd[i][:-1],
                       2 * h * (WT + W1) * u, scratch)
            lows.append(res[0])
            if i == 0:
                sigma_par = res[1]
        for i in range(halves):
            res = call(functools.partial(post_body, Z, t, p, u),
                       [shape(t + p, u)] * Q + [jax.ShapeDtypeStruct((1, u), F32)],
                       sides + [tops[i], lows[i], own[i], ku[i][-1], kd[i][-1]], 2 * (g + h) ** 2 * u,
                       [pltpu.VMEM((g, u), F32), pltpu.VMEM((h, u), F32),
                        pltpu.VMEM((g, u), BF16), pltpu.VMEM((h, u), BF16)])
            var.append(res[Q])
            outs += [res[0]] + [in_group(res[k], k) for k in range(1, Q)]

        var = jnp.concatenate(var, axis=1)
        var = [var] + [between(var, [(a, (a + m) % Z) for a in range(Z)])
                       for m in range(1, Z)]
        var = call(functools.partial(line_sum_body, Z), jax.ShapeDtypeStruct((1, w), F32),
                   [where] + var, 1, [pltpu.VMEM((max(Z, 8), w), F32)])
        var = [var] + [in_group(var, k) for k in range(1, Q)]
        cross_kid_top, cross_kid_par = call(
            functools.partial(out_body, t, p, u, halves, per_kid),
            [shape(kids, t, W2), shape(kids, p, W2)], [where] + outs, 1)
        variance_kid = call(functools.partial(variance_body, w, per_kid),
                            jax.ShapeDtypeStruct((kids, W2), F32), [where, after(dvar_kid, cross_kid_top)] + var, 1)
        return cross_par, sigma_par, cross_kid_top, cross_kid_par, variance_kid

    return choose


def solution(mesh):
    rows = P(("parts", "row"), None)
    kid = P("parts", "row", None)
    return jax.shard_map(
        make_shards(mesh.shape["row"]),
        mesh=mesh,
        in_specs=(rows, rows, rows, kid, kid, P("parts", None), P("parts", None),
                  P("parts", None, None), P("parts", None, None)),
        out_specs=(rows, rows, kid, kid, P("parts", None)),
        check_vma=False,
    )
```

```python
import functools

import jax
import jax.numpy as jnp
from jax import lax
from jax.experimental import pallas as pl
from jax.experimental.pallas import tpu as pltpu
from jax.sharding import PartitionSpec as P


F32 = jnp.float32
BF16 = jnp.bfloat16
Q = 4
ORDER = (0, 2, 1, 3)
EXTRA = 16


def mask_rows(mask, rows, width, height, position):
    high = height // mask.shape[-2]
    wide = width // mask.shape[-1]
    if high % rows == 0:
        picked = lax.dynamic_slice_in_dim(mask, position * rows // high, 1, axis=mask.ndim - 2)
    else:
        index = (position * rows + jnp.arange(rows, dtype=jnp.int32)) // high
        picked = jnp.take(mask, index, axis=mask.ndim - 2)
    return jnp.repeat(picked.astype(BF16), wide, axis=-1)


def dot(a, b):
    return jnp.dot(a, b, preferred_element_type=F32)


def dot_t(a, b):
    return lax.dot_general(a, b, (((0,), (0,)), ((), ())), preferred_element_type=F32)


def after(x, *deps):
    return lax.optimization_barrier((x,) + deps)[0]


def split3(x):
    high = x.astype(BF16)
    rest = x - high.astype(F32)
    mid = rest.astype(BF16)
    return high, mid, (rest - mid.astype(F32)).astype(BF16)


def call(body, out_shape, args, flops, scratch=(), smem=1):
    size = sum(a.size * a.dtype.itemsize for a in args)
    vmem = pl.BlockSpec(memory_space=pltpu.VMEM)
    return pl.pallas_call(
        body,
        out_shape=out_shape,
        in_specs=[pl.BlockSpec(memory_space=pltpu.SMEM)] * smem + [vmem] * (len(args) - smem),
        out_specs=jax.tree.map(lambda _: vmem, out_shape),
        scratch_shapes=list(scratch),
        cost_estimate=pl.CostEstimate(flops=flops, bytes_accessed=size, transcendentals=0),
        compiler_params=pltpu.CompilerParams(vmem_limit_bytes=20 * 2 ** 20),
    )(*args)


def place(own, ups, downs, z, Z):
    out = [(own, z, None)]
    for s, (u, d) in enumerate(zip(ups, downs), 1):
        out.append((u, z - s, z >= s))
        out.append((d, z + s, z + s < Z))
    return out


def when(flag, f):
    if flag is None:
        f()
    else:
        pl.when(flag)(f)


def fill(slots, z, q, Z, full, step, off, rows):
    n = (len(slots) - 1) // 2
    for x, zi, flag in place(slots[0], slots[1:1 + n], slots[1 + n:], z, Z):
        def put(x=x, zi=zi):
            for k in range(Q):
                at = pl.multiple_of((zi * Q + (q ^ k)) * rows, rows)
                full[pl.ds(at, rows), :] = x[k * step + off:k * step + off + rows, :]

        when(flag, put)


def par_body(t, v, wide, high, where_ref, mask_ref, x_ref, *outs):
    pos, q = where_ref[2], where_ref[1]
    row = pos * t // high
    step = min(v, wide)
    for k in range(Q):
        peer = q ^ k
        for c in range(0, v, step):
            keep = mask_ref[row, (peer * v + c) // wide] != 0
            x = x_ref[:, pl.ds(pl.multiple_of(peer * v + c, step), step)]
            outs[k][:, c:c + step] = jnp.where(keep, x, jnp.zeros_like(x))


def kid_body(t, p, u, halves, per_kid, wide, high_t, high_p, where_ref, mt_ref, mp_ref, xt_ref,
             xp_ref, *outs):
    pos, q = where_ref[2], where_ref[1]
    step = min(u, wide)
    for k in range(Q):
        peer = q ^ k
        one = peer // per_kid
        for i in range(halves):
            for c in range(0, u, step):
                col = (peer % per_kid) * (u * halves) + i * u + c
                at = pl.ds(pl.multiple_of(col, step), step)
                for m_ref, x_ref, high, r, lo in ((mt_ref, xt_ref, high_t, t, 0),
                                                  (mp_ref, xp_ref, high_p, p, t)):
                    keep = m_ref[one, pos * r // high, col // wide] != 0
                    x = x_ref[one, :, at]
                    outs[k][i, lo:lo + r, c:c + step] = jnp.where(keep, x, jnp.zeros_like(x))


def cross_body(Z, t, where_ref, sa_ref, sb_ref, *refs):
    slots, out_ref, full = refs[:-2], refs[-2], refs[-1]
    z, q = where_ref[0], where_ref[1]
    fill(slots, z, q, Z, full, t, 0, t)
    for i, k in enumerate(ORDER):
        s = (sa_ref, sb_ref)[i // 2]
        at = pl.ds(pl.multiple_of((q ^ k) * t, t), t)
        out_ref[at, :] = dot(s[(i % 2) * t:(i % 2 + 1) * t, :], full[...]).astype(BF16)


def sigma_body(Z, t, p, v, where_ref, da_ref, db_ref, ta_ref, tb_ref, *refs):
    slots, out_ref, full, acc = refs[:-3], refs[-3], refs[-2], refs[-1]
    z, q = where_ref[0], where_ref[1]
    g = Q * t
    fill(slots, z, q, Z, full, t, 0, t)
    cols = pl.ds(pl.multiple_of(q * v, v), v)
    for i, k in enumerate(ORDER):
        d = (da_ref, db_ref)[i // 2]
        at = pl.ds(pl.multiple_of((q ^ k) * p, p), p)
        acc[at, :] = d[(i % 2) * p:(i % 2 + 1) * p, cols]
    for i, k in enumerate(ORDER):
        x = (ta_ref, tb_ref)[i // 2]
        at = pl.ds(pl.multiple_of((q ^ k) * g, g), g)
        acc[...] += dot_t(x[(i % 2) * g:(i % 2 + 1) * g, :], full[at, :])
    out_ref[...] = acc[...].astype(BF16)


def pre_body(Z, t, p, u, v, first, where_ref, sa_ref, sb_ref, ca_ref, cb_ref, *refs):
    refs = list(refs)
    kp, kt = refs.pop(), refs.pop()
    if first:
        cross_ref = refs.pop()
    top = refs.pop()
    slots = refs
    z, q = where_ref[0], where_ref[1]
    g, h = Q * t, Q * p
    far = jnp.where(z + Z - 1 < Z, z + Z - 1, z - Z + 1)

    def clear():
        kt[pl.ds(pl.multiple_of(far * g, g), g), :] = jnp.zeros((g, u), BF16)
        kp[pl.ds(pl.multiple_of(far * h, h), h), :] = jnp.zeros((h, u), BF16)

    pl.when(far >= 0)(clear)
    fill(slots, z, q, Z, kt, t + p, 0, t)
    fill(slots, z, q, Z, kp, t + p, t, p)
    for i, k in enumerate(ORDER):
        peer = q ^ k
        s = (sa_ref, sb_ref)[i // 2]
        c = dot(s[(i % 2) * t:(i % 2 + 1) * t, :], kt[...])
        for j, m in enumerate(ORDER):
            x = (ca_ref, cb_ref)[j // 2]
            at = pl.ds(pl.multiple_of((q ^ m) * v, v), v)
            mine = pl.ds(pl.multiple_of((j % 2) * g + peer * t, t), t)
            c = c + dot(x[mine, :], kp[at, :])
        top[i * t:(i + 1) * t, :] = c
    if first:
        for j, m in enumerate(ORDER):
            at = pl.ds(pl.multiple_of((q ^ m) * v, v), v)
            x = (ca_ref, cb_ref)[j // 2]
            cross_ref[:, at] = x[pl.ds(pl.multiple_of((j % 2) * g + q * t, t), t), :]


def low_body(Z, t, p, u, v, first, where_ref, ta_ref, tb_ref, pa_ref, pb_ref, *refs):
    refs = list(refs)
    kp, kt = refs.pop(), refs.pop()
    if first:
        sp_ref = refs.pop()
    low = refs.pop()
    slots = refs
    z, q = where_ref[0], where_ref[1]
    g, h = Q * t, Q * p
    far = jnp.where(z + Z - 1 < Z, z + Z - 1, z - Z + 1)

    def clear():
        kt[pl.ds(pl.multiple_of(far * g, g), g), :] = jnp.zeros((g, u), BF16)
        kp[pl.ds(pl.multiple_of(far * h, h), h), :] = jnp.zeros((h, u), BF16)

    pl.when(far >= 0)(clear)
    fill(slots, z, q, Z, kt, t + p, 0, t)
    fill(slots, z, q, Z, kp, t + p, t, p)
    for i, k in enumerate(ORDER):
        x = (ta_ref, tb_ref)[i // 2]
        at = pl.ds(pl.multiple_of((q ^ k) * g, g), g)
        part = dot_t(x[(i % 2) * g:(i % 2 + 1) * g, :], kt[at, :])
        low[...] = part if i == 0 else low[...] + part
        x = (pa_ref, pb_ref)[i // 2]
        at = pl.ds(pl.multiple_of((q ^ k) * v, v), v)
        low[...] += dot(x[(i % 2) * h:(i % 2 + 1) * h, :], kp[at, :])
    if first:
        for j, m in enumerate(ORDER):
            at = pl.ds(pl.multiple_of((q ^ m) * v, v), v)
            x = (pa_ref, pb_ref)[j // 2]
            sp_ref[:, at] = x[pl.ds(pl.multiple_of((j % 2) * h + q * p, p), p), :]


def post_body(Z, t, p, u, where_ref, sa_ref, sb_ref, ca_ref, cb_ref, ta_ref, tb_ref,
              pa_ref, pb_ref, top_in, low_in, own, up_ref, down_ref, *refs):
    outs, (var_ref, top, low, kt, kp) = refs[:Q], refs[Q:]
    z, q = where_ref[0], where_ref[1]
    g, h = Q * t, Q * p
    top[...] = top_in[...]
    low[...] = low_in[...]
    for x, zi, flag in ((up_ref, z - (Z - 1), z >= Z - 1), (down_ref, z + (Z - 1), z <= 0)):
        def put(x=x, zi=zi):
            for k in range(Q):
                at = pl.ds(pl.multiple_of((q ^ k) * t, t), t)
                kt[at, :] = x[k * (t + p):k * (t + p) + t, :]
                at = pl.ds(pl.multiple_of((q ^ k) * p, p), p)
                kp[at, :] = x[k * (t + p) + t:(k + 1) * (t + p), :]
            cols = pl.ds(pl.multiple_of(zi * g, g), g)
            for j, m in enumerate(ORDER):
                def add(j=j):
                    side, lo = j // 2, j % 2
                    low[...] += dot_t((ta_ref, tb_ref)[side][lo * g:(lo + 1) * g, :], kt[...])
                    low[...] += dot((pa_ref, pb_ref)[side][lo * h:(lo + 1) * h, :], kp[...])
                    for i, k in enumerate(ORDER):
                        mine = pl.ds(pl.multiple_of(lo * g + (q ^ k) * t, t), t)
                        s = (sa_ref, sb_ref)[i // 2]
                        rows = slice(i * t, (i + 1) * t)
                        top[rows, :] += (
                            dot(s[(i % 2) * t:(i % 2 + 1) * t, cols], kt[...])
                            + dot((ca_ref, cb_ref)[side][mine, :], kp[...]))

                pl.when(zi == q ^ m)(add)

        pl.when(flag)(put)
    var = jnp.zeros((1, u), F32)
    for i, k in enumerate(ORDER):
        c = top[i * t:(i + 1) * t, :].astype(BF16)
        outs[k][:t, :] = c
        x = own[k * (t + p):k * (t + p) + t, :]
        var = var + jnp.sum(x.astype(F32) * c.astype(F32), axis=0, keepdims=True)
        c = low[pl.ds(pl.multiple_of((q ^ k) * p, p), p), :].astype(BF16)
        outs[k][t:, :] = c
        x = own[k * (t + p) + t:(k + 1) * (t + p), :]
        var = var + jnp.sum(x.astype(F32) * c.astype(F32), axis=0, keepdims=True)
    var_ref[...] = var


def out_body(t, p, u, halves, per_kid, where_ref, dvar_ref, *refs):
    ins, (top_ref, low_ref, var_ref) = refs[:-3], refs[-3:]
    q = where_ref[1]
    w = u * halves
    for k in range(Q):
        peer = q ^ k
        one = peer // per_kid
        for i in range(halves):
            x = ins[Q + i * Q + k]
            at = pl.ds(pl.multiple_of((peer % per_kid) * w + i * u, u), u)
            top_ref[one, :, at] = x[:t, :]
            low_ref[one, :, at] = x[t:t + p, :]
        at = pl.ds(pl.multiple_of((peer % per_kid) * w, w), w)
        row = pl.ds(one, 1)
        var_ref[row, at] = dvar_ref[row, at] + ins[k][...]


def line_sum_body(Z, where_ref, *refs):
    ins, out_ref, rows = refs[:-2], refs[-2], refs[-1]
    for m in range(Z):
        rows[pl.ds(lax.rem(where_ref[0] - m + Z, Z), 1), :] = ins[m][...]
    total = rows[0:1, :]
    for k in range(1, Z):
        total = total + rows[k:k + 1, :]
    out_ref[...] = total


def make_shards(n):
    Z = n // Q

    def plain(sigma_top, panel_par, dinv_par, panel_kid_top, panel_kid_par, dvar_kid,
              mask_par, mask_kid_top, mask_kid_par):
        t, WT = sigma_top.shape
        p, W1 = dinv_par.shape
        kids, _, W2 = panel_kid_top.shape
        per_kid = Q // kids
        w = kids * W2 // Q
        v = W1 // Q
        g, h = Q * t, Q * p
        halves = 2
        u = w // halves
        pos = lax.axis_index("row")
        z = pos // Q
        q = pos % Q

        def permute(x, pairs):
            return lax.ppermute(x, "row", pairs)

        def in_group(x, k):
            pairs = [(a * Q + b, a * Q + (b ^ k)) for a in range(Z) for b in range(Q)]
            return permute(x, pairs)

        def between(x, zpairs):
            return permute(x, [(a * Q + b, c * Q + b) for a, c in zpairs for b in range(Q)])

        def unxor(pieces, at=None):
            at = q if at is None else at
            pieces = list(pieces)
            bit = 1
            while bit < Q:
                flag = (at & bit) != 0
                pieces = [jnp.where(flag, pieces[k ^ bit], pieces[k]) for k in range(Q)]
                bit *= 2
            return pieces

        def pair_gather(x):
            first = jnp.concatenate([x, in_group(x, 2)], axis=0)
            return first, in_group(first, 1)

        def gather4(x):
            first, second = pair_gather(x)
            r = x.shape[0]
            return unxor([first[:r], second[:r], first[r:], second[r:]])

        def hop(x, s, way):
            if way > 0:
                return between(x, [(a, a + 1) for a in range(s - 1, Z - 1)])
            return between(x, [(a, a - 1) for a in range(1, Z - s + 1)])

        def pieces_of(c):
            own = lax.dynamic_index_in_dim(c, q, 0, keepdims=False)
            return [own] + [in_group(lax.dynamic_index_in_dim(c, q ^ k, 0, keepdims=False), k) for k in range(1, Q)]

        def assemble(own, ups, downs):
            r = own.shape[0]
            full = jnp.zeros(((Z + 1) * r,) + own.shape[1:], own.dtype)
            for x, zi, flag in place(own, ups, downs, z, Z):
                zi = zi if flag is None else jnp.where(flag, zi, Z)
                full = lax.dynamic_update_slice(full, x, (zi * r, 0))
            return full[:Z * r]

        par_d = panel_par * mask_rows(mask_par, t, W1, WT, pos)
        par_g = jnp.concatenate(
            unxor(pieces_of(par_d.reshape(t, Q, v).transpose(1, 0, 2))), axis=0)

        def chunks(x):
            r = x.shape[1]
            return x.reshape(kids, r, per_kid, w).transpose(0, 2, 1, 3).reshape(Q, r, w)

        kt_d = after(panel_kid_top, par_d) * mask_rows(mask_kid_top, t, W2, WT, pos)
        kp_d = panel_kid_par * mask_rows(mask_kid_par, p, W2, W1, pos)
        kid = unxor(pieces_of(jnp.concatenate([chunks(kt_d), chunks(kp_d)], axis=1)))
        kid_g = jnp.concatenate([x[:t] for x in kid] + [x[t:] for x in kid], axis=0)
        own = [kid_g[:, i * u:(i + 1) * u] for i in range(halves)]

        pu, pd = [], []
        ku, kd = [[] for _ in own], [[] for _ in own]
        for s in range(1, Z):
            pu.append(hop(pu[-1] if pu else par_g, s, 1))
            pd.append(hop(pd[-1] if pd else par_g, s, -1))
        for s in range(1, Z):
            for i in range(halves):
                ku[i].append(hop(ku[i][-1] if s > 1 else own[i], s, 1))
                kd[i].append(hop(kd[i][-1] if s > 1 else own[i], s, -1))

        sig_a, sig_b = pair_gather(after(sigma_top, kid_g))
        dinv_pieces = gather4(after(dinv_par, sig_a))
        dinv_c = jnp.concatenate(
            [lax.dynamic_slice(x, (0, q * v), (p, v)) for x in dinv_pieces], axis=0)

        par = assemble(par_g, pu, pd)
        cross_c = jnp.concatenate([dot(sig_a, par), dot(sig_b, par)], 0).astype(BF16)

        if Z == Q:
            turn = permute(cross_c, [(a * Q + b, b * Q + a) for a in range(Z) for b in range(Q)])
            turn = jnp.concatenate(unxor([turn[ORDER.index(k) * t:(ORDER.index(k) + 1) * t]
                                          for k in range(Q)], z), axis=0)
            turned = jnp.concatenate(gather4(turn), axis=0)

        ca, cb = pair_gather(cross_c)
        chunk = (ca[:g], cb[:g], ca[g:], cb[g:])

        def cross_rows(r):
            at = [ORDER.index(r ^ k) * t for k in range(Q)]
            return jnp.concatenate(
                unxor([chunk[k][at[k]:at[k] + t] for k in range(Q)]), axis=1)

        cross_par = cross_rows(0)
        cross_g = jnp.concatenate([cross_par] + [cross_rows(r) for r in ORDER[1:]], axis=0)
        if Z != Q:
            turn = lax.all_to_all(cross_par, "row", split_axis=1, concat_axis=0, tiled=True)
            turned = jnp.concatenate(gather4(turn), axis=1)

        sigma_c = (dinv_c + dot_t(turned, par)).astype(BF16)
        sigma_g = jnp.concatenate(gather4(sigma_c), axis=1)
        sigma_par = lax.dynamic_slice(sigma_g, (q * p, 0), (p, W1))

        def final(i):
            full = assemble(own[i], ku[i], kd[i]).reshape(Z, g + h, u)
            kt, kp = full[:, :g].reshape(WT, u), full[:, g:].reshape(W1, u)
            sig = jnp.concatenate([sig_a, sig_b], 0)
            top = (dot(sig, kt) + dot(cross_g, kp)).astype(BF16).reshape(Q, t, u)
            low = (dot_t(turned, kt) + dot(sigma_g, kp)).astype(BF16).reshape(Q, p, u)
            top = jnp.stack([top[ORDER.index(k)] for k in range(Q)])
            low = jnp.stack([lax.dynamic_index_in_dim(low, q ^ k, 0, False) for k in range(Q)])
            mine = own[i].astype(F32)
            var = jnp.zeros((1, u), F32)
            for k in range(Q):
                x = lax.dynamic_slice(mine, ((q ^ k) * t, 0), (t, u))
                y = lax.dynamic_slice(mine, (g + (q ^ k) * p, 0), (p, u))
                var = var + jnp.sum(x * top[k].astype(F32), 0, keepdims=True)
                var = var + jnp.sum(y * low[k].astype(F32), 0, keepdims=True)
            tail = jnp.concatenate(split3(var) + (jnp.zeros((EXTRA - 3, u), BF16),), axis=0)
            return jnp.concatenate([top, low, jnp.broadcast_to(tail, (Q, EXTRA, u))], axis=1)

        outs = []
        for i in range(halves):
            c = final(i)
            outs.append(unxor([c[0]] + [in_group(c[k], k) for k in range(1, Q)]))

        def whole(first, last):
            x = jnp.stack([jnp.stack([outs[i][j][first:last] for i in range(halves)], 0)
                           for j in range(Q)], 0)
            x = x.reshape(kids, per_kid, halves, last - first, u)
            return x.transpose(0, 3, 1, 2, 4).reshape(kids, last - first, W2)

        cross_kid_top = whole(0, t)
        cross_kid_par = whole(t, t + p)
        three = whole(t + p, t + p + 3).astype(F32)
        part = three[:, 0] + three[:, 1] + three[:, 2]
        sums = jnp.zeros((Z, kids, W2), F32)
        sums = lax.dynamic_update_slice(sums, part[None], (z, 0, 0))
        for m in range(1, Z):
            other = between(part, [(a, (a + m) % Z) for a in range(Z)])
            sums = lax.dynamic_update_slice(sums, other[None], ((z - m) % Z, 0, 0))
        variance_kid = dvar_kid + jnp.sum(sums, axis=0)
        return cross_par, sigma_par, cross_kid_top, cross_kid_par, variance_kid

    def choose(*args):
        sigma_top, _, dinv_par, kid_top = args[:4]
        t, WT = sigma_top.shape
        p, W1 = dinv_par.shape
        masks = args[6:]
        u = kid_top.shape[0] * kid_top.shape[2] // Q // 2
        wide = kid_top.shape[2] // masks[1].shape[-1]
        good = (Z == Q and t % 16 == 0 and p % 16 == 0 and (W1 // Q) % 128 == 0 and u % 128 == 0
                and (WT // masks[0].shape[0]) % t == 0 and (W1 // masks[2].shape[1]) % p == 0
                and wide % 128 == 0 and Q % kid_top.shape[0] == 0)
        return (fast if good else plain)(*args)

    def fast(sigma_top, panel_par, dinv_par, panel_kid_top, panel_kid_par, dvar_kid,
             mask_par, mask_kid_top, mask_kid_par):
        t, WT = sigma_top.shape
        p, W1 = dinv_par.shape
        kids, _, W2 = panel_kid_top.shape
        per_kid = Q // kids
        w = kids * W2 // Q
        v = W1 // Q
        g, h = Q * t, Q * p
        halves = 2
        u = w // halves
        pos = lax.axis_index("row")
        z = pos // Q
        q = pos % Q
        where = jnp.stack([z, q, pos]).astype(jnp.int32)

        def permute(x, pairs):
            return lax.ppermute(x, "row", pairs)

        def in_group(x, k):
            pairs = [(a * Q + b, a * Q + (b ^ k)) for a in range(Z) for b in range(Q)]
            return permute(x, pairs)

        def between(x, zpairs):
            return permute(x, [(a * Q + b, c * Q + b) for a, c in zpairs for b in range(Q)])

        def pair_gather(x):
            first = jnp.concatenate([x, in_group(x, 2)], axis=0)
            return first, in_group(first, 1)

        def hop(x, s, way):
            if way > 0:
                return between(x, [(a, a + 1) for a in range(s - 1, Z - 1)])
            return between(x, [(a, a - 1) for a in range(1, Z - s + 1)])

        def shape(*dims):
            return jax.ShapeDtypeStruct(dims, BF16)

        wide = W1 // mask_par.shape[1]
        sent = call(functools.partial(par_body, t, v, wide, WT // mask_par.shape[0]),
                    [shape(t, v)] * Q, [where, mask_par, panel_par], 1, smem=2)
        par_g = jnp.concatenate(
            [sent[0]] + [in_group(sent[k], k) for k in range(1, Q)], axis=0)

        wide = W2 // mask_kid_top.shape[2]
        sent = call(functools.partial(kid_body, t, p, u, halves, per_kid, wide,
                                      WT // mask_kid_top.shape[1], W1 // mask_kid_par.shape[1]),
                    [shape(halves, t + p, u)] * Q,
                    [where, mask_kid_top, mask_kid_par, after(panel_kid_top, sent[0]),
                     panel_kid_par], 1, smem=3)
        got = [sent[0]] + [in_group(sent[k], k) for k in range(1, Q)]
        own = [jnp.concatenate([x[i] for x in got], axis=0) for i in range(halves)]

        pu, pd = [], []
        ku, kd = [[] for _ in own], [[] for _ in own]
        for s in range(1, Z):
            pu.append(hop(pu[-1] if pu else par_g, s, 1))
            pd.append(hop(pd[-1] if pd else par_g, s, -1))
        for s in range(1, Z):
            for i in range(halves):
                ku[i].append(hop(ku[i][-1] if s > 1 else own[i], s, 1))
                kd[i].append(hop(kd[i][-1] if s > 1 else own[i], s, -1))

        sig_a, sig_b = pair_gather(sigma_top)
        dinv_a, dinv_b = pair_gather(dinv_par)

        cross_c = call(functools.partial(cross_body, Z, t), shape(g, v),
                       [where, sig_a, sig_b, par_g] + pu + pd, 2 * g * WT * v,
                       [pltpu.VMEM((WT, v), BF16)])
        turn = permute(cross_c, [(a * Q + b, b * Q + a) for a in range(Z) for b in range(Q)])
        turned_a, turned_b = pair_gather(turn)
        cross_a, cross_b = pair_gather(cross_c)

        sigma_c = call(functools.partial(sigma_body, Z, t, p, v), shape(h, v),
                       [where, dinv_a, dinv_b, turned_a, turned_b, par_g] + pu + pd,
                       2 * h * WT * v, [pltpu.VMEM((WT, v), BF16), pltpu.VMEM((h, v), F32)])
        sp_a, sp_b = pair_gather(sigma_c)

        sides = [where, sig_a, sig_b, cross_a, cross_b, turned_a, turned_b, sp_a, sp_b]
        wide32 = [jax.ShapeDtypeStruct((g, u), F32), jax.ShapeDtypeStruct((h, u), F32)]
        outs, var, tops, lows = [], [], [], []
        scratch = [pltpu.VMEM((WT, u), BF16), pltpu.VMEM((W1, u), BF16)]
        for i in range(halves):
            res = call(functools.partial(pre_body, Z, t, p, u, v, i == 0),
                       wide32[:1] + ([shape(t, W1)] if i == 0 else []),
                       [where, sig_a, sig_b, cross_a, cross_b, own[i]] + ku[i][:-1] + kd[i][:-1],
                       2 * g * (WT + W1) * u, scratch)
            tops.append(res[0])
            if i == 0:
                cross_par = res[1]
        for i in range(halves):
            res = call(functools.partial(low_body, Z, t, p, u, v, i == 0),
                       wide32[1:] + ([shape(p, W1)] if i == 0 else []),
                       [where, turned_a, turned_b, sp_a, sp_b, own[i]] + ku[i][:-1] + kd[i][:-1],
                       2 * h * (WT + W1) * u, scratch)
            lows.append(res[0])
            if i == 0:
                sigma_par = res[1]
        for i in range(halves):
            res = call(functools.partial(post_body, Z, t, p, u),
                       [shape(t + p, u)] * Q + [jax.ShapeDtypeStruct((1, u), F32)],
                       sides + [tops[i], lows[i], own[i], ku[i][-1], kd[i][-1]], 2 * (g + h) ** 2 * u,
                       [pltpu.VMEM((g, u), F32), pltpu.VMEM((h, u), F32),
                        pltpu.VMEM((g, u), BF16), pltpu.VMEM((h, u), BF16)])
            var.append(res[Q])
            outs += [res[0]] + [in_group(res[k], k) for k in range(1, Q)]

        var = jnp.concatenate(var, axis=1)
        var = [var] + [between(var, [(a, (a + m) % Z) for a in range(Z)])
                       for m in range(1, Z)]
        var = call(functools.partial(line_sum_body, Z), jax.ShapeDtypeStruct((1, w), F32),
                   [where] + var, 1, [pltpu.VMEM((max(Z, 8), w), F32)])
        var = [var] + [in_group(var, k) for k in range(1, Q)]
        cross_kid_top, cross_kid_par, variance_kid = call(
            functools.partial(out_body, t, p, u, halves, per_kid),
            [shape(kids, t, W2), shape(kids, p, W2), jax.ShapeDtypeStruct((kids, W2), F32)],
            [where, dvar_kid] + var + outs, 1)
        return cross_par, sigma_par, cross_kid_top, cross_kid_par, variance_kid

    return choose


def solution(mesh):
    rows = P(("parts", "row"), None)
    kid = P("parts", "row", None)
    return jax.shard_map(
        make_shards(mesh.shape["row"]),
        mesh=mesh,
        in_specs=(rows, rows, rows, kid, kid, P("parts", None), P("parts", None),
                  P("parts", None, None), P("parts", None, None)),
        out_specs=(rows, rows, kid, kid, P("parts", None)),
        check_vma=False,
    )
```
